32 devices in a mesh: dp: 1 (over z), sp: 32 (over y, x, core).
Axes of the slice: x: 4, y: 4, z: 1, core: 2. Of those that a mesh axis runs over, the one named last changes fastest.
The devices are a block of a 4x4x8 slice.
Arguments:
- tokens: bfloat16 [2, 8192, 2048], P('dp', 'sp')
- expert_ids: int32 [2, 8192, 8], P('dp', 'sp')
- w_query: bfloat16 [2048, 32, 128], replicated
- w_key: bfloat16 [2048, 4, 128], replicated
- w_value: bfloat16 [2048, 4, 128], replicated
- w_out: bfloat16 [32, 128, 2048], replicated
- w_router: bfloat16 [2048, 128], replicated
Outputs:
- output 1: bfloat16 [2, 8192, 2048], P('dp', 'sp')
- output 2: bfloat16 [2, 128, 1024, 2048], P('dp', 'sp')
All inputs are finite; a program needn't handle non-finite values.
Results may differ from the reference program's by a relative error of at most 0.0135601.
Values are sent between devices in bfloat16 or wider.
A program may use at most 768 MiB of HBM per device.

```python
import math
import jax
import jax.numpy as jnp
from jax import lax

GROUP_SIZE = 32
TOK_DEV = 256
D_MODEL = 2048
NUM_HEADS = 32
KV_HEADS = 4
HEAD_DIM = 128
EXPERTS = 128
TOP_K = 8
MICRO_BATCHES = 2
SEQ_LEN = GROUP_SIZE * TOK_DEV
GROUP_Q = NUM_HEADS // KV_HEADS
CAPACITY = 2 * TOK_DEV * TOP_K // EXPERTS
Q_BLOCK = min(SEQ_LEN, 128)
SCORE_GAIN = math.sqrt(0.8 * math.log(SEQ_LEN))


def draw_routing(rng_key):
    hot_key, score_key = jax.random.split(rng_key)
    hot_expert = jax.random.randint(hot_key, (MICRO_BATCHES, GROUP_SIZE, 1, 1), 0, EXPERTS)
    raw_score = jax.random.randint(score_key, (MICRO_BATCHES, GROUP_SIZE, TOK_DEV, EXPERTS), 0, 2 ** 20)
    expert_pos = jnp.arange(EXPERTS)
    boosted = raw_score + jnp.where(expert_pos == hot_expert, 2 ** 20, 0)
    ranked = boosted * EXPERTS + expert_pos
    chosen = lax.top_k(ranked, TOP_K)[1]
    return chosen.reshape(MICRO_BATCHES, SEQ_LEN, TOP_K).astype(jnp.int32)


def setup_inputs(seed: int = 0, part: int = 0) -> dict:
    base_key = jax.random.key(seed)
    part_key = jax.random.fold_in(base_key, part)
    tok_key, route_key = jax.random.split(part_key)
    wq_key, wk_key, wv_key, wo_key, wr_key = jax.random.split(base_key, 5)
    q_width = NUM_HEADS * HEAD_DIM
    tokens = jax.random.normal(tok_key, (MICRO_BATCHES, SEQ_LEN, D_MODEL), jnp.float32)
    w_query = jax.random.normal(wq_key, (D_MODEL, NUM_HEADS, HEAD_DIM), jnp.float32) * (SCORE_GAIN / math.sqrt(D_MODEL))
    w_key = jax.random.normal(wk_key, (D_MODEL, KV_HEADS, HEAD_DIM), jnp.float32) / math.sqrt(D_MODEL)
    w_value = jax.random.normal(wv_key, (D_MODEL, KV_HEADS, HEAD_DIM), jnp.float32) / math.sqrt(D_MODEL)
    w_out = jax.random.normal(wo_key, (NUM_HEADS, HEAD_DIM, D_MODEL), jnp.float32) / math.sqrt(q_width)
    w_router = jax.random.normal(wr_key, (D_MODEL, EXPERTS), jnp.float32) * (2.0 / math.sqrt(D_MODEL))
    return {
        'tokens': tokens.astype(jnp.bfloat16),
        'expert_ids': draw_routing(route_key),
        'w_query': w_query.astype(jnp.bfloat16),
        'w_key': w_key.astype(jnp.bfloat16),
        'w_value': w_value.astype(jnp.bfloat16),
        'w_out': w_out.astype(jnp.bfloat16),
        'w_router': w_router.astype(jnp.bfloat16),
    }


def attend_micro(tok_mb, w_query, w_key, w_value, w_out):
    q_width = NUM_HEADS * HEAD_DIM
    kv_width = KV_HEADS * HEAD_DIM
    queries = jnp.dot(tok_mb, w_query.reshape(D_MODEL, q_width), preferred_element_type=jnp.float32).astype(jnp.bfloat16)
    queries = queries.reshape(SEQ_LEN, KV_HEADS, GROUP_Q, HEAD_DIM).astype(jnp.float32)
    key_rows = jnp.dot(tok_mb, w_key.reshape(D_MODEL, kv_width), preferred_element_type=jnp.float32).astype(jnp.bfloat16)
    key_rows = key_rows.reshape(SEQ_LEN, KV_HEADS, HEAD_DIM).astype(jnp.float32)
    value_rows = jnp.dot(tok_mb, w_value.reshape(D_MODEL, kv_width), preferred_element_type=jnp.float32).astype(jnp.bfloat16)
    value_rows = value_rows.reshape(SEQ_LEN, KV_HEADS, HEAD_DIM).astype(jnp.float32)
    key_pos = jnp.arange(SEQ_LEN)

    def one_block(blk_start):
        q_blk = lax.dynamic_slice_in_dim(queries, blk_start, Q_BLOCK, 0)
        scores = jnp.einsum('qhgd,khd->hgqk', q_blk, key_rows) / math.sqrt(HEAD_DIM)
        q_pos = blk_start + jnp.arange(Q_BLOCK)
        scores = jnp.where(q_pos[:, None] >= key_pos[None, :], scores, -jnp.inf)
        attn_probs = jax.nn.softmax(scores, axis=-1).astype(jnp.bfloat16).astype(jnp.float32)
        return jnp.einsum('hgqk,khd->qhgd', attn_probs, value_rows).astype(jnp.bfloat16)

    blocks = lax.map(one_block, jnp.arange(SEQ_LEN // Q_BLOCK) * Q_BLOCK)
    attn_out = blocks.reshape(SEQ_LEN, q_width)
    attn_proj = jnp.dot(attn_out, w_out.reshape(q_width, D_MODEL), preferred_element_type=jnp.float32)
    return (tok_mb.astype(jnp.float32) + attn_proj).astype(jnp.bfloat16)


def dispatch_micro(hid_mb, ids_mb, w_router):
    logits = jnp.dot(hid_mb, w_router, preferred_element_type=jnp.float32)
    gate_w = jax.nn.softmax(jnp.take_along_axis(logits, ids_mb, axis=1), axis=-1)
    scaled = (gate_w[:, :, None] * hid_mb[:, None, :].astype(jnp.float32)).astype(jnp.bfloat16)
    pair_ids = ids_mb.reshape(GROUP_SIZE, TOK_DEV * TOP_K)
    pair_hot = (pair_ids[:, :, None] == jnp.arange(EXPERTS)).astype(jnp.int32)
    slot_rank = jnp.sum((jnp.cumsum(pair_hot, axis=1) - pair_hot) * pair_hot, axis=-1)
    source = jnp.arange(GROUP_SIZE)[:, None]
    dest_row = jnp.where(slot_rank < CAPACITY, source * CAPACITY + slot_rank, GROUP_SIZE * CAPACITY)
    zero_rows = jnp.zeros((EXPERTS, GROUP_SIZE * CAPACITY, D_MODEL), jnp.bfloat16)
    return zero_rows.at[pair_ids.reshape(-1), dest_row.reshape(-1)].set(scaled.reshape(SEQ_LEN * TOP_K, D_MODEL), mode='drop')


def reference(tokens, expert_ids, w_query, w_key, w_value, w_out, w_router):
    def one_micro(mb_args):
        tok_mb, ids_mb = mb_args
        hid_mb = attend_micro(tok_mb, w_query, w_key, w_value, w_out)
        return hid_mb, dispatch_micro(hid_mb, ids_mb, w_router)

    hidden, expert_rows = lax.map(one_micro, (tokens, expert_ids))
    return hidden, expert_rows
```

```python
import functools
import math
import jax
import jax.numpy as jnp
from jax import lax
from jax.experimental import pallas as pl
from jax.experimental.pallas import tpu as pltpu
from jax.sharding import PartitionSpec as P

F32 = jnp.float32
BF16 = jnp.bfloat16
ANY = pl.BlockSpec(memory_space=pl.ANY)


def attention_kernel(first, q_block, per_step, blk, q_ref, kv_ref, *rest):
    o_ref, m_ref, l_ref, acc_ref = rest[-4:]
    i = pl.program_id(0) + first
    ring = kv_ref.shape[0]
    hd = q_ref.shape[1]
    step_keys = per_step * blk
    scale = math.log2(math.e) / math.sqrt(hd)
    m_ref[...] = jnp.full(m_ref.shape, -jnp.inf, F32)
    l_ref[...] = jnp.zeros(l_ref.shape, F32)
    acc_ref[...] = jnp.zeros(acc_ref.shape, F32)

    def step(j, masked):
        keys, values = [], []
        for u in range(per_step):
            b = j * per_step + u
            keys.append(kv_ref[lax.rem(b, ring), lax.div(b, ring), :, :hd])
            values.append(kv_ref[lax.rem(b, ring), lax.div(b, ring), :, hd:])
        k = jnp.concatenate(keys, axis=0)
        v = jnp.concatenate(values, axis=0)
        s = lax.dot_general(q_ref[...], k, (((1,), (1,)), ((), ())), preferred_element_type=F32)
        if masked:
            row = lax.broadcasted_iota(jnp.int32, s.shape, 0)
            col = lax.broadcasted_iota(jnp.int32, s.shape, 1)
            s = jnp.where(row >= col, s, -jnp.inf)
        top = s[:, :hd]
        for u in range(1, step_keys // hd):
            top = jnp.maximum(top, s[:, u * hd:(u + 1) * hd])
        m_old = m_ref[...]
        m_new = jnp.maximum(m_old, jnp.max(top, axis=1, keepdims=True))
        m_ref[...] = m_new
        alpha = jnp.exp2((m_old - m_new) * scale)
        m_scaled = m_new * scale
        parts = [jnp.exp2(s[:, u * hd:(u + 1) * hd] * scale - m_scaled) for u in range(step_keys // hd)]
        total = parts[0]
        for part in parts[1:]:
            total = total + part
        l_ref[...] = l_ref[...] * alpha + total
        p = jnp.concatenate([part.astype(BF16) for part in parts], axis=1)
        acc_ref[...] = acc_ref[...] * alpha + jnp.dot(p, v, preferred_element_type=F32)

    lax.fori_loop(0, i, lambda j, c: (step(j, False), c)[1], 0)
    step(i, True)
    o_ref[...] = (acc_ref[...] / jnp.sum(l_ref[...], axis=1, keepdims=True)).astype(BF16)


def attention(q, kv, lo, hi, q_block, into=None, after=()):
    seq, hd = q.shape
    ring, rows, blk, _ = kv.shape
    steps = hi - lo
    extra = list(after) + ([into] if into is not None else [])
    frac = (hi * hi - lo * lo) * q_block * q_block / 2
    return pl.pallas_call(
        functools.partial(attention_kernel, lo, q_block, q_block // blk, blk),
        grid=(steps,),
        in_specs=[
            pl.BlockSpec((q_block, hd), lambda i: (i + lo, 0)),
            pl.BlockSpec((ring, rows, blk, 2 * hd), lambda i: (0, 0, 0, 0)),
        ] + [ANY] * len(extra),
        out_specs=pl.BlockSpec((q_block, hd), lambda i: (i + lo, 0)),
        out_shape=jax.ShapeDtypeStruct((seq, hd), BF16),
        scratch_shapes=[pltpu.VMEM((q_block, hd), F32)] * 3,
        input_output_aliases={1 + len(extra): 0} if into is not None else {},
        cost_estimate=pl.CostEstimate(flops=int(16 * hd * frac), bytes_accessed=int(seq * hd * 8), transcendentals=int(frac)),
        name='attend',
    )(q, kv, *extra)


def project_kernel(heads_blk, pair, o_ref, w_ref, x_ref, ids_ref, wr_ref, *rest):
    h_ref, g_ref, acc_ref = rest[-3:]
    step = pl.program_id(0)

    @pl.when(step == 0)
    def _():
        acc_ref[...] = jnp.zeros(acc_ref.shape, F32)

    o = jnp.concatenate([o_ref[u] for u in range(heads_blk)], axis=1)
    w = w_ref[...].reshape(heads_blk * w_ref.shape[1], w_ref.shape[2])
    acc_ref[...] += jnp.dot(o, w, preferred_element_type=F32)

    @pl.when(step == pl.num_programs(0) - 1)
    def _():
        h = (x_ref[...].astype(F32) + acc_ref[...]).astype(BF16)
        h_ref[...] = h
        logits = jnp.dot(h, wr_ref[...], preferred_element_type=F32)
        expert = lax.broadcasted_iota(jnp.int32, logits.shape, 1)
        chosen = ids_ref[:, 0:1] == expert
        for u in range(1, ids_ref.shape[1]):
            chosen = jnp.logical_or(chosen, ids_ref[:, u:u + 1] == expert)
        picked = jnp.where(chosen, logits, -jnp.inf)
        e = jnp.exp(picked - jnp.max(picked, axis=1, keepdims=True))
        g_ref[...] = (e / jnp.sum(e, axis=1, keepdims=True)).T


def project(o, w_out, x, ids, w_router, after=()):
    heads, tok, hd = o.shape
    width = w_out.shape[2]
    experts = w_router.shape[1]
    heads_blk = min(heads, 8)
    return pl.pallas_call(
        functools.partial(project_kernel, heads_blk, 2),
        grid=(heads // heads_blk,),
        in_specs=[
            pl.BlockSpec((heads_blk, tok, hd), lambda i: (i, 0, 0)),
            pl.BlockSpec((heads_blk, hd, width), lambda i: (i, 0, 0)),
            pl.BlockSpec((tok, width), lambda i: (0, 0)),
            pl.BlockSpec((tok, ids.shape[1]), lambda i: (0, 0)),
            pl.BlockSpec((width, experts), lambda i: (0, 0)),
        ] + [ANY] * len(after),
        out_specs=[
            pl.BlockSpec((tok, width), lambda i: (0, 0)),
            pl.BlockSpec((experts, tok), lambda i: (0, 0)),
        ],
        out_shape=[jax.ShapeDtypeStruct((tok, width), BF16), jax.ShapeDtypeStruct((experts, tok), F32)],
        scratch_shapes=[pltpu.VMEM((tok, width), F32)],
        cost_estimate=pl.CostEstimate(flops=2 * tok * heads * hd * width, bytes_accessed=heads * hd * width * 2, transcendentals=0),
        name='project',
    )(o, w_out, x, ids, w_router, *after)


def rows_kernel(h_ref, rank_ref, gate_ref, *rest):
    out_ref = rest[-1]
    experts, cap = out_ref.shape[1], out_ref.shape[2]
    tok = h_ref.shape[0]
    slot = lax.broadcasted_iota(jnp.int32, (cap, tok), 0).astype(F32)
    hot, gate = [], []
    for e in range(experts):
        here = rank_ref[0, 0, e:e + 1, :] == slot
        hot.append(jnp.where(here, 1.0, 0.0))
        gate.append(jnp.sum(jnp.where(here, gate_ref[0, e:e + 1, :], 0.0), axis=1, keepdims=True))
    select = jnp.concatenate(hot, axis=0).astype(BF16)
    gates = jnp.concatenate(gate, axis=0)
    rows = jnp.dot(select, h_ref[...], preferred_element_type=F32)
    out_ref[0] = (rows * gates).astype(BF16).reshape(experts, cap, h_ref.shape[1])


def expert_rows(h_all, ranks, gates, micro, cap, into=None, after=()):
    sources, n_micro, experts, tok = ranks.shape
    width = h_all.shape[1]
    extra = list(after) + ([into] if into is not None else [])
    return pl.pallas_call(
        rows_kernel,
        grid=(sources,),
        in_specs=[
            pl.BlockSpec((tok, width), lambda s: (s, 0)),
            pl.BlockSpec((1, 1, experts, tok), lambda s: (s, micro, 0, 0)),
            pl.BlockSpec((1, experts, tok), lambda s: (s, 0, 0)),
        ] + [ANY] * len(extra),
        out_specs=pl.BlockSpec((1, experts, cap, width), lambda s: (micro, 0, s, 0)),
        out_shape=jax.ShapeDtypeStruct((n_micro, experts, sources * cap, width), BF16),
        input_output_aliases={2 + len(extra): 0} if into is not None else {},
        cost_estimate=pl.CostEstimate(flops=2 * sources * experts * cap * tok * width, bytes_accessed=2 * sources * (tok + experts * cap) * width, transcendentals=0),
        name='expert_rows',
    )(h_all, ranks, gates, *extra)


def slot_ranks(ids, experts, cap):
    tok = ids.shape[1]
    hot = jnp.any(ids[:, None, :, :] == jnp.arange(experts)[None, :, None, None], axis=-1)
    earlier = (jnp.arange(tok)[:, None] < jnp.arange(tok)[None, :]).astype(BF16)
    rank = jnp.einsum('met,ts->mes', hot.astype(BF16), earlier, preferred_element_type=F32)
    return jnp.where(jnp.logical_and(hot, rank < cap), rank, -1.0)


def solution(mesh):
    groups = mesh.shape['sp']

    def local_step(tokens, expert_ids, w_query, w_key, w_value, w_out, w_router):
        n_micro, tok, width = tokens.shape
        top_k = expert_ids.shape[2]
        heads, hd = w_query.shape[1:]
        kv_heads = w_key.shape[1]
        experts = w_router.shape[1]
        own = experts // groups
        cap = 2 * tok * top_k // experts
        share = groups // kv_heads
        seq = groups * tok
        columns = [[r + share * y for y in range(kv_heads)] for r in range(share)]
        rows = [[r + share * y for r in range(share)] for y in range(kv_heads)]
        q_block = min(2 * tok, seq)
        n_blk = seq // q_block

        def swap(a, **kw):
            return lax.all_to_all(a, 'sp', 0, 0, tiled=True, **kw)

        w_kv = jnp.concatenate([w_key, w_value], axis=2)
        kv = jnp.einsum('mtd,dhk->mhtk', tokens, w_kv, preferred_element_type=F32).astype(BF16)
        kv_held = []
        for m in range(n_micro):
            mine = swap(kv[m], axis_index_groups=columns)
            gathered = lax.all_gather(mine, 'sp', axis=0, axis_index_groups=rows)
            kv_held.append(gathered.reshape(share, kv_heads, tok, 2 * hd))
        ranks = slot_ranks(expert_ids, experts, cap).reshape(n_micro, groups, own, tok)
        ranks = swap(ranks.transpose(1, 0, 2, 3))
        q = jnp.einsum('mtd,dhk->mhtk', tokens, w_query, preferred_element_type=F32).astype(BF16)
        q_held = [swap(q[m]).reshape(seq, hd) for m in range(n_micro)]

        hidden, buffers, gathered = [], None, []
        attn = attention(q_held[0], kv_held[0], 0, n_blk, q_block)
        for m in range(n_micro):
            o = swap(attn.reshape(groups, tok, hd))
            part = None
            if m + 1 < n_micro:
                cut = (5 * n_blk) // 8
                part = attention(q_held[m + 1], kv_held[m + 1], 0, cut, q_block)
            h, gate = project(o, w_out, tokens[m], expert_ids[m], w_router, after=() if part is None else (part,))
            hidden.append(h)
            h_all = lax.all_gather(h, 'sp', axis=0, tiled=True)
            gates = swap(gate.reshape(groups, own, tok))
            gathered.append((h_all, gates))
            if part is not None:
                attn = attention(q_held[m + 1], kv_held[m + 1], cut, n_blk, q_block, into=part, after=(h,))
        for m in range(n_micro):
            h_all, gates = gathered[m]
            buffers = expert_rows(h_all, ranks, gates, m, cap, into=buffers, after=(attn,) if m == 0 else ())
        return jnp.stack(hidden), buffers

    return jax.shard_map(
        local_step,
        mesh=mesh,
        in_specs=(P('dp', 'sp', None), P('dp', 'sp', None), P(), P(), P(), P(), P()),
        out_specs=(P('dp', 'sp', None), P('dp', 'sp', None, None)),
        check_vma=False,
    )
```

```python
import functools
import math
import jax
import jax.numpy as jnp
from jax import lax
from jax.experimental import pallas as pl
from jax.experimental.pallas import tpu as pltpu
from jax.sharding import PartitionSpec as P

F32 = jnp.float32
BF16 = jnp.bfloat16
ANY = pl.BlockSpec(memory_space=pl.ANY)


def attention_kernel(first, q_ref, kv_ref, *rest):
    o_ref, q_rows, m_ref, l_ref, acc_ref = rest[-5:]
    i = pl.program_id(0) + first
    ring = kv_ref.shape[0]
    blk = kv_ref.shape[3]
    per_q, hd = q_ref.shape[0], q_ref.shape[1]
    scale = math.log2(math.e) / math.sqrt(hd)
    for u in range(per_q):
        q_rows[u * blk:(u + 1) * blk, :] = q_ref[u].T
    m_ref[...] = jnp.full(m_ref.shape, -jnp.inf, F32)
    l_ref[...] = jnp.zeros(l_ref.shape, F32)
    acc_ref[...] = jnp.zeros(acc_ref.shape, F32)

    half = q_rows.shape[0] // 2

    def step(start, count, spans, masked):
        keys, values = [], []
        for u in range(count):
            b = start + u
            keys.append(kv_ref[lax.rem(b, ring), lax.div(b, ring), :hd, :])
            values.append(kv_ref[lax.rem(b, ring), lax.div(b, ring), hd:, :])
        k = jnp.concatenate(keys, axis=1)
        v = jnp.concatenate(values, axis=1)
        scores = [jnp.dot(q_rows[span, :], k, preferred_element_type=F32) for span in spans]
        for span, s in zip(spans, scores):
            if masked:
                row = lax.broadcasted_iota(jnp.int32, s.shape, 0) + span.start
                col = lax.broadcasted_iota(jnp.int32, s.shape, 1)
                s = jnp.where(row >= col, s, -jnp.inf)
            pieces = [s[:, u:u + hd] for u in range(0, count * blk, hd)]
            m_old = m_ref[span, :]
            top = functools.reduce(jnp.maximum, pieces)
            m_new = jnp.maximum(m_old, jnp.max(top, axis=1, keepdims=True))
            m_ref[span, :] = m_new
            alpha = jnp.exp2((m_old - m_new) * scale)
            m_scaled = m_new * scale
            parts = [jnp.exp2(piece * scale - m_scaled) for piece in pieces]
            l_ref[span, :] = l_ref[span, :] * alpha + functools.reduce(jnp.add, parts)
            p = jnp.concatenate([part.astype(BF16) for part in parts], axis=1)
            o = lax.dot_general(p, v, (((1,), (1,)), ((), ())), preferred_element_type=F32)
            acc_ref[span, :] = acc_ref[span, :] * alpha + o

    def full(j, carry):
        step(j * per_q, per_q, [slice(0, half), slice(half, 2 * half)], False)
        return carry

    lax.fori_loop(0, i, full, 0)
    step(i * per_q, per_q, [slice(0, half), slice(half, 2 * half)], True)
    o_ref[...] = (acc_ref[...] / jnp.sum(l_ref[...], axis=1, keepdims=True)).astype(BF16)


def attention(q, kv, lo, hi, per_q, into=None, after=()):
    n_src, hd, blk = q.shape
    ring, rows = kv.shape[:2]
    q_block = per_q * blk
    seq = n_src * blk
    extra = list(after) + ([into] if into is not None else [])
    pairs = (hi * hi - lo * lo) * q_block * q_block / 2
    return pl.pallas_call(
        functools.partial(attention_kernel, lo),
        grid=(hi - lo,),
        in_specs=[
            pl.BlockSpec((per_q, hd, blk), lambda i: (i + lo, 0, 0)),
            pl.BlockSpec((ring, rows, 2 * hd, blk), lambda i: (0, 0, 0, 0)),
        ] + [ANY] * len(extra),
        out_specs=pl.BlockSpec((q_block, hd), lambda i: (i + lo, 0)),
        out_shape=jax.ShapeDtypeStruct((seq, hd), BF16),
        scratch_shapes=[pltpu.VMEM((q_block, hd), BF16)] + [pltpu.VMEM((q_block, hd), F32)] * 3,
        input_output_aliases={1 + len(extra): 0} if into is not None else {},
        cost_estimate=pl.CostEstimate(flops=int(4 * hd * pairs * 2), bytes_accessed=int(seq * hd * 8), transcendentals=int(pairs)),
        name='attend',
    )(q, kv, *extra)


def project_kernel(heads_blk, parts, o_ref, w_ref, x_ref, ids_ref, wr_ref, *rest):
    *part_refs, h_ref, g_ref, acc_ref = rest[-3 - parts:]
    step = pl.program_id(0)

    @pl.when(step == 0)
    def _():
        acc_ref[...] = jnp.zeros(acc_ref.shape, F32)

    o = jnp.concatenate([o_ref[u] for u in range(heads_blk)], axis=1)
    tile = min(w_ref.shape[2], 512)

    def add(c, carry):
        cols = pl.ds(pl.multiple_of(c * tile, tile), tile)
        w = w_ref[:, :, cols].reshape(heads_blk * w_ref.shape[1], tile)
        acc_ref[:, cols] += jnp.dot(o, w, preferred_element_type=F32)
        return carry

    lax.fori_loop(0, w_ref.shape[2] // tile, add, 0)

    @pl.when(step == pl.num_programs(0) - 1)
    def _():
        h = (x_ref[...].astype(F32) + acc_ref[...]).astype(BF16)
        h_ref[...] = h
        for u, part_ref in enumerate(part_refs):
            size = part_ref.shape[1]
            part_ref[...] = h[:, u * size:(u + 1) * size]
        logits = jnp.dot(h, wr_ref[...], preferred_element_type=F32)
        expert = lax.broadcasted_iota(jnp.int32, logits.shape, 1)
        chosen = ids_ref[:, 0:1] == expert
        for u in range(1, ids_ref.shape[1]):
            chosen = jnp.logical_or(chosen, ids_ref[:, u:u + 1] == expert)
        picked = jnp.where(chosen, logits, -jnp.inf)
        e = jnp.exp(picked - jnp.max(picked, axis=1, keepdims=True))
        g_ref[...] = (e / jnp.sum(e, axis=1, keepdims=True)).T


def project(o, w_out, x, ids, w_router, parts, after=()):
    heads, tok, hd = o.shape
    width = w_out.shape[2]
    experts = w_router.shape[1]
    heads_blk = min(heads, 8)
    return pl.pallas_call(
        functools.partial(project_kernel, heads_blk, parts),
        grid=(heads // heads_blk,),
        in_specs=[
            pl.BlockSpec((heads_blk, tok, hd), lambda i: (i, 0, 0)),
            pl.BlockSpec((heads_blk, hd, width), lambda i: (i, 0, 0)),
            pl.BlockSpec((tok, width), lambda i: (0, 0)),
            pl.BlockSpec((tok, ids.shape[1]), lambda i: (0, 0)),
            pl.BlockSpec((width, experts), lambda i: (0, 0)),
        ] + [ANY] * len(after),
        out_specs=[pl.BlockSpec((tok, width // parts), lambda i: (0, 0))] * parts + [
            pl.BlockSpec((tok, width), lambda i: (0, 0)),
            pl.BlockSpec((experts, tok), lambda i: (0, 0)),
        ],
        out_shape=[jax.ShapeDtypeStruct((tok, width // parts), BF16)] * parts + [
            jax.ShapeDtypeStruct((tok, width), BF16), jax.ShapeDtypeStruct((experts, tok), F32)],
        scratch_shapes=[pltpu.VMEM((tok, width), F32)],
        cost_estimate=pl.CostEstimate(flops=2 * tok * heads * hd * width, bytes_accessed=heads * hd * width * 2, transcendentals=0),
        name='project',
    )(o, w_out, x, ids, w_router, *after)


def rows_kernel(h_ref, rank_ref, gate_ref, *rest):
    out_ref = rest[-1]
    experts = out_ref.shape[1]
    some, _, tok = gate_ref.shape
    cap = out_ref.shape[2] // some
    slot = lax.broadcasted_iota(jnp.int32, (cap, tok), 0).astype(F32)

    def source(u, carry):
        hot, gate = [], []
        for e in range(experts):
            here = rank_ref[u, 0, e:e + 1, :] == slot
            hot.append(jnp.where(here, 1.0, 0.0))
            gate.append(jnp.sum(jnp.where(here, gate_ref[u, e:e + 1, :], 0.0), axis=1, keepdims=True))
        select = jnp.concatenate(hot, axis=0).astype(BF16)
        gates = jnp.concatenate(gate, axis=0)
        rows = jnp.dot(select, h_ref[pl.ds(pl.multiple_of(u * tok, tok), tok), :], preferred_element_type=F32)
        slots = pl.ds(pl.multiple_of(u * cap, cap), cap)
        out_ref[0, :, slots, :] = (rows * gates).astype(BF16).reshape(experts, cap, rows.shape[1])
        return carry

    lax.fori_loop(0, some, source, 0)


def expert_rows(h_all, ranks, gates, micro, cap, width, column, into=None, after=()):
    sources, n_micro, experts, tok = ranks.shape
    part = h_all.shape[1]
    some = min(sources, 4)
    extra = list(after) + ([into] if into is not None else [])
    return pl.pallas_call(
        rows_kernel,
        grid=(sources // some,),
        in_specs=[
            pl.BlockSpec((some * tok, part), lambda s: (s, 0)),
            pl.BlockSpec((some, 1, experts, tok), lambda s: (s, micro, 0, 0)),
            pl.BlockSpec((some, experts, tok), lambda s: (s, 0, 0)),
        ] + [ANY] * len(extra),
        out_specs=pl.BlockSpec((1, experts, some * cap, part), lambda s: (micro, 0, s, column)),
        out_shape=jax.ShapeDtypeStruct((n_micro, experts, sources * cap, width), BF16),
        input_output_aliases={2 + len(extra): 0} if into is not None else {},
        cost_estimate=pl.CostEstimate(flops=2 * sources * experts * cap * tok * part, bytes_accessed=2 * sources * (tok + experts * cap) * part, transcendentals=0),
        name='expert_rows',
    )(h_all, ranks, gates, *extra)


def slot_ranks(ids, experts, cap):
    tok = ids.shape[1]
    hot = jnp.any(ids[:, None, :, :] == jnp.arange(experts)[None, :, None, None], axis=-1)
    earlier = (jnp.arange(tok)[:, None] < jnp.arange(tok)[None, :]).astype(BF16)
    rank = jnp.einsum('met,ts->mes', hot.astype(BF16), earlier, preferred_element_type=F32)
    return jnp.where(jnp.logical_and(hot, rank < cap), rank, -1.0)


def solution(mesh):
    groups = mesh.shape['sp']

    def local_step(tokens, expert_ids, w_query, w_key, w_value, w_out, w_router):
        n_micro, tok, width = tokens.shape
        top_k = expert_ids.shape[2]
        heads, hd = w_query.shape[1:]
        kv_heads = w_key.shape[1]
        experts = w_router.shape[1]
        own = experts // groups
        cap = 2 * tok * top_k // experts
        share = groups // kv_heads
        seq = groups * tok
        columns = [[r + share * y for y in range(kv_heads)] for r in range(share)]
        rows = [[r + share * y for r in range(share)] for y in range(kv_heads)]
        per_q = min(4, groups)
        n_blk = groups // per_q

        def swap(a, **kw):
            return lax.all_to_all(a, 'sp', 0, 0, tiled=True, **kw)

        def queries(m, x):
            return jnp.einsum('td,dhk->hkt', x, w_query, preferred_element_type=F32).astype(BF16)

        w_kv = jnp.concatenate([w_key, w_value], axis=2)
        kv = jnp.einsum('mtd,dhk->hmkt', tokens, w_kv, preferred_element_type=F32).astype(BF16)
        ranks = slot_ranks(expert_ids, experts, cap).reshape(n_micro, groups, own, tok).transpose(1, 0, 2, 3)
        mine = swap(kv, axis_index_groups=columns)
        q = queries(0, tokens[0])
        mine, q, ranks = lax.optimization_barrier((mine, q, ranks))
        ranks = swap(ranks)
        kv_held, q_held = [], []
        for m in range(n_micro):
            if m > 0:
                x, _ = lax.optimization_barrier((tokens[m], q))
                q = queries(m, x)
                q, _ = lax.optimization_barrier((q, q_held[-1]))
            gathered = lax.all_gather(mine[:, m], 'sp', axis=0, axis_index_groups=rows)
            kv_held.append(gathered.reshape(share, kv_heads, 2 * hd, tok))
            q_held.append(swap(q))

        hidden, buffers, gathered = [], None, []
        attn = attention(q_held[0], kv_held[0], 0, n_blk, per_q)
        for m in range(n_micro):
            o = swap(attn.reshape(groups, tok, hd))
            part = None
            last = m + 1 == n_micro
            if not last:
                cut = (5 * n_blk) // 8
                part = attention(q_held[m + 1], kv_held[m + 1], 0, cut, per_q)
            parts = 2 if last else 1
            *pieces, h, gate = project(o, w_out, tokens[m], expert_ids[m], w_router, parts, after=() if last else (part,))
            hidden.append(h)
            pieces = [lax.all_gather(piece, 'sp', axis=0, tiled=True) for piece in pieces]
            gates = swap(gate.reshape(groups, own, tok))
            gathered.append((pieces, gates))
            if not last:
                attn = attention(q_held[m + 1], kv_held[m + 1], cut, n_blk, per_q, into=part, after=(h,))
        for m in range(n_micro):
            pieces, gates = gathered[m]
            for c, piece in enumerate(pieces):
                buffers = expert_rows(piece, ranks, gates, m, cap, width, c, into=buffers, after=(attn,) if m == 0 else ())
        return jnp.stack(hidden), buffers

    return jax.shard_map(
        local_step,
        mesh=mesh,
        in_specs=(P('dp', 'sp', None), P('dp', 'sp', None), P(), P(), P(), P(), P()),
        out_specs=(P('dp', 'sp', None), P('dp', 'sp', None, None)),
        check_vma=False,
    )
```

```python
import functools
import math
import jax
import jax.numpy as jnp
from jax import lax
from jax.experimental import pallas as pl
from jax.experimental.pallas import tpu as pltpu
from jax.sharding import PartitionSpec as P

F32 = jnp.float32
BF16 = jnp.bfloat16
ANY = pl.BlockSpec(memory_space=pl.ANY)


def attention_kernel(first, q_ref, kv_ref, *rest):
    o_ref, q_rows, m_ref, l_ref, acc_ref = rest[-5:]
    i = pl.program_id(0) + first
    ring = kv_ref.shape[0]
    blk = kv_ref.shape[3]
    per_q, hd = q_ref.shape[0], q_ref.shape[1]
    scale = math.log2(math.e) / math.sqrt(hd)
    for u in range(per_q):
        q_rows[u * blk:(u + 1) * blk, :] = q_ref[u].T
    m_ref[...] = jnp.full(m_ref.shape, -jnp.inf, F32)
    l_ref[...] = jnp.zeros(l_ref.shape, F32)
    acc_ref[...] = jnp.zeros(acc_ref.shape, F32)

    half = q_rows.shape[0] // 2

    def step(start, count, spans, masked):
        keys, values = [], []
        for u in range(count):
            b = start + u
            keys.append(kv_ref[lax.rem(b, ring), lax.div(b, ring), :hd, :])
            values.append(kv_ref[lax.rem(b, ring), lax.div(b, ring), hd:, :])
        k = jnp.concatenate(keys, axis=1)
        v = jnp.concatenate(values, axis=1)
        scores = [jnp.dot(q_rows[span, :], k, preferred_element_type=F32) for span in spans]
        for span, s in zip(spans, scores):
            if masked:
                row = lax.broadcasted_iota(jnp.int32, s.shape, 0) + span.start
                col = lax.broadcasted_iota(jnp.int32, s.shape, 1)
                s = jnp.where(row >= col, s, -jnp.inf)
            pieces = [s[:, u:u + hd] for u in range(0, count * blk, hd)]
            m_old = m_ref[span, :]
            top = functools.reduce(jnp.maximum, pieces)
            m_new = jnp.maximum(m_old, jnp.max(top, axis=1, keepdims=True))
            m_ref[span, :] = m_new
            alpha = jnp.exp2((m_old - m_new) * scale)
            m_scaled = m_new * scale
            parts = [jnp.exp2(piece * scale - m_scaled) for piece in pieces]
            l_ref[span, :] = l_ref[span, :] * alpha + functools.reduce(jnp.add, parts)
            p = jnp.concatenate([part.astype(BF16) for part in parts], axis=1)
            o = lax.dot_general(p, v, (((1,), (1,)), ((), ())), preferred_element_type=F32)
            acc_ref[span, :] = acc_ref[span, :] * alpha + o

    def full(j, carry):
        step(j * per_q, per_q, [slice(0, half), slice(half, 2 * half)], False)
        return carry

    lax.fori_loop(0, i, full, 0)
    step(i * per_q, per_q, [slice(0, half), slice(half, 2 * half)], True)
    o_ref[...] = (acc_ref[...] / jnp.sum(l_ref[...], axis=1, keepdims=True)).astype(BF16)


def attention(q, kv, lo, hi, per_q, into=None, after=()):
    n_src, hd, blk = q.shape
    ring, rows = kv.shape[:2]
    q_block = per_q * blk
    seq = n_src * blk
    extra = list(after) + ([into] if into is not None else [])
    pairs = (hi * hi - lo * lo) * q_block * q_block / 2
    return pl.pallas_call(
        functools.partial(attention_kernel, lo),
        grid=(hi - lo,),
        in_specs=[
            pl.BlockSpec((per_q, hd, blk), lambda i: (i + lo, 0, 0)),
            pl.BlockSpec((ring, rows, 2 * hd, blk), lambda i: (0, 0, 0, 0)),
        ] + [ANY] * len(extra),
        out_specs=pl.BlockSpec((q_block, hd), lambda i: (i + lo, 0)),
        out_shape=jax.ShapeDtypeStruct((seq, hd), BF16),
        scratch_shapes=[pltpu.VMEM((q_block, hd), BF16)] + [pltpu.VMEM((q_block, hd), F32)] * 3,
        input_output_aliases={1 + len(extra): 0} if into is not None else {},
        cost_estimate=pl.CostEstimate(flops=int(4 * hd * pairs * 2), bytes_accessed=int(seq * hd * 8), transcendentals=int(pairs)),
        name='attend',
    )(q, kv, *extra)


def project_kernel(heads_blk, parts, o_ref, w_ref, x_ref, ids_ref, wr_ref, *rest):
    *part_refs, h_ref, g_ref, acc_ref = rest[-3 - parts:]
    step = pl.program_id(0)

    @pl.when(step == 0)
    def _():
        acc_ref[...] = jnp.zeros(acc_ref.shape, F32)

    o = jnp.concatenate([o_ref[u] for u in range(heads_blk)], axis=1)
    tile = min(w_ref.shape[2], 512)

    def add(c, carry):
        cols = pl.ds(pl.multiple_of(c * tile, tile), tile)
        w = w_ref[:, :, cols].reshape(heads_blk * w_ref.shape[1], tile)
        acc_ref[:, cols] += jnp.dot(o, w, preferred_element_type=F32)
        return carry

    lax.fori_loop(0, w_ref.shape[2] // tile, add, 0)

    @pl.when(step == pl.num_programs(0) - 1)
    def _():
        h = (x_ref[...].astype(F32) + acc_ref[...]).astype(BF16)
        h_ref[...] = h
        for u, part_ref in enumerate(part_refs):
            size = part_ref.shape[1]
            part_ref[...] = h[:, u * size:(u + 1) * size]
        logits = jnp.dot(h, wr_ref[...], preferred_element_type=F32)
        expert = lax.broadcasted_iota(jnp.int32, logits.shape, 1)
        chosen = ids_ref[:, 0:1] == expert
        for u in range(1, ids_ref.shape[1]):
            chosen = jnp.logical_or(chosen, ids_ref[:, u:u + 1] == expert)
        picked = jnp.where(chosen, logits, -jnp.inf)
        e = jnp.exp(picked - jnp.max(picked, axis=1, keepdims=True))
        g_ref[...] = (e / jnp.sum(e, axis=1, keepdims=True)).T


def project(o, w_out, x, ids, w_router, parts, after=()):
    heads, tok, hd = o.shape
    width = w_out.shape[2]
    experts = w_router.shape[1]
    heads_blk = min(heads, 8)
    return pl.pallas_call(
        functools.partial(project_kernel, heads_blk, parts),
        grid=(heads // heads_blk,),
        in_specs=[
            pl.BlockSpec((heads_blk, tok, hd), lambda i: (i, 0, 0)),
            pl.BlockSpec((heads_blk, hd, width), lambda i: (i, 0, 0)),
            pl.BlockSpec((tok, width), lambda i: (0, 0)),
            pl.BlockSpec((tok, ids.shape[1]), lambda i: (0, 0)),
            pl.BlockSpec((width, experts), lambda i: (0, 0)),
        ] + [ANY] * len(after),
        out_specs=[pl.BlockSpec((tok, width // parts), lambda i: (0, 0))] * parts + [
            pl.BlockSpec((tok, width), lambda i: (0, 0)),
            pl.BlockSpec((experts, tok), lambda i: (0, 0)),
        ],
        out_shape=[jax.ShapeDtypeStruct((tok, width // parts), BF16)] * parts + [
            jax.ShapeDtypeStruct((tok, width), BF16), jax.ShapeDtypeStruct((experts, tok), F32)],
        scratch_shapes=[pltpu.VMEM((tok, width), F32)],
        cost_estimate=pl.CostEstimate(flops=2 * tok * heads * hd * width, bytes_accessed=heads * hd * width * 2, transcendentals=0),
        name='project',
    )(o, w_out, x, ids, w_router, *after)


def rows_kernel(h_ref, rank_ref, gate_ref, *rest):
    out_ref = rest[-1]
    experts = out_ref.shape[1]
    some, _, tok = gate_ref.shape
    cap = out_ref.shape[2] // some
    slot = lax.broadcasted_iota(jnp.int32, (cap, tok), 0).astype(F32)

    def source(u, carry):
        hot, gate = [], []
        for e in range(experts):
            here = rank_ref[u, 0, e:e + 1, :] == slot
            hot.append(jnp.where(here, 1.0, 0.0))
            gate.append(jnp.sum(jnp.where(here, gate_ref[u, e:e + 1, :], 0.0), axis=1, keepdims=True))
        select = jnp.concatenate(hot, axis=0).astype(BF16)
        gates = jnp.concatenate(gate, axis=0)
        rows = jnp.dot(select, h_ref[pl.ds(pl.multiple_of(u * tok, tok), tok), :], preferred_element_type=F32)
        slots = pl.ds(pl.multiple_of(u * cap, cap), cap)
        out_ref[0, :, slots, :] = (rows * gates).astype(BF16).reshape(experts, cap, rows.shape[1])
        return carry

    lax.fori_loop(0, some, source, 0)


def expert_rows(h_all, ranks, gates, micro, cap, width, column, into=None, after=()):
    sources, n_micro, experts, tok = ranks.shape
    part = h_all.shape[1]
    some = min(sources, 4)
    extra = list(after) + ([into] if into is not None else [])
    return pl.pallas_call(
        rows_kernel,
        grid=(sources // some,),
        in_specs=[
            pl.BlockSpec((some * tok, part), lambda s: (s, 0)),
            pl.BlockSpec((some, 1, experts, tok), lambda s: (s, micro, 0, 0)),
            pl.BlockSpec((some, experts, tok), lambda s: (s, 0, 0)),
        ] + [ANY] * len(extra),
        out_specs=pl.BlockSpec((1, experts, some * cap, part), lambda s: (micro, 0, s, column)),
        out_shape=jax.ShapeDtypeStruct((n_micro, experts, sources * cap, width), BF16),
        input_output_aliases={2 + len(extra): 0} if into is not None else {},
        cost_estimate=pl.CostEstimate(flops=2 * sources * experts * cap * tok * part, bytes_accessed=2 * sources * (tok + experts * cap) * part, transcendentals=0),
        name='expert_rows',
    )(h_all, ranks, gates, *extra)


def slot_ranks(ids, experts, cap):
    tok = ids.shape[1]
    hot = jnp.any(ids[:, None, :, :] == jnp.arange(experts)[None, :, None, None], axis=-1)
    earlier = (jnp.arange(tok)[:, None] < jnp.arange(tok)[None, :]).astype(BF16)
    rank = jnp.einsum('met,ts->mes', hot.astype(BF16), earlier, preferred_element_type=F32)
    return jnp.where(jnp.logical_and(hot, rank < cap), rank, -1.0)


def solution(mesh):
    groups = mesh.shape['sp']

    def local_step(tokens, expert_ids, w_query, w_key, w_value, w_out, w_router):
        n_micro, tok, width = tokens.shape
        top_k = expert_ids.shape[2]
        heads, hd = w_query.shape[1:]
        kv_heads = w_key.shape[1]
        experts = w_router.shape[1]
        own = experts // groups
        cap = 2 * tok * top_k // experts
        share = groups // kv_heads
        seq = groups * tok
        columns = [[r + share * y for y in range(kv_heads)] for r in range(share)]
        rows = [[r + share * y for r in range(share)] for y in range(kv_heads)]
        per_q = min(4, groups)
        n_blk = groups // per_q

        def swap(a, **kw):
            return lax.all_to_all(a, 'sp', 0, 0, tiled=True, **kw)

        w_kv = jnp.concatenate([w_key, w_value], axis=2)
        kv = jnp.einsum('mtd,dhk->hmkt', tokens, w_kv, preferred_element_type=F32).astype(BF16)
        ranks = slot_ranks(expert_ids, experts, cap).reshape(n_micro, groups, own, tok).transpose(1, 0, 2, 3)
        mine = swap(kv, axis_index_groups=columns)
        queries = jnp.einsum('mtd,dhk->hmkt', tokens, w_query, preferred_element_type=F32).astype(BF16)
        mine, queries, ranks = lax.optimization_barrier((mine, queries, ranks))
        ranks = swap(ranks)
        kv_held, q_held = [], []
        for m in range(n_micro):
            q = queries[:, m]
            if m > 0:
                q, _ = lax.optimization_barrier((q, q_held[-1]))
            gathered = lax.all_gather(mine[:, m], 'sp', axis=0, axis_index_groups=rows)
            kv_held.append(gathered.reshape(share, kv_heads, 2 * hd, tok))
            q_held.append(swap(q))

        hidden, buffers, gathered = [], None, []
        attn = attention(q_held[0], kv_held[0], 0, n_blk, per_q)
        for m in range(n_micro):
            o = swap(attn.reshape(groups, tok, hd))
            part = None
            last = m + 1 == n_micro
            if not last:
                cut = (5 * n_blk) // 8
                part = attention(q_held[m + 1], kv_held[m + 1], 0, cut, per_q)
            parts = 1
            *pieces, h, gate = project(o, w_out, tokens[m], expert_ids[m], w_router, parts, after=() if last else (part,))
            hidden.append(h)
            pieces = [lax.all_gather(piece, 'sp', axis=0, tiled=True) for piece in pieces]
            gates = swap(gate.reshape(groups, own, tok))
            gathered.append((pieces, gates))
            if not last:
                attn = attention(q_held[m + 1], kv_held[m + 1], cut, n_blk, per_q, into=part, after=(h,))
        for m in range(n_micro):
            pieces, gates = gathered[m]
            for c, piece in enumerate(pieces):
                buffers = expert_rows(piece, ranks, gates, m, cap, width, c, into=buffers, after=(attn,) if m == 0 else ())
        return jnp.stack(hidden), buffers

    return jax.shard_map(
        local_step,
        mesh=mesh,
        in_specs=(P('dp', 'sp', None), P('dp', 'sp', None), P(), P(), P(), P(), P()),
        out_specs=(P('dp', 'sp', None), P('dp', 'sp', None, None)),
        check_vma=False,
    )
```

```python
import functools
import math
import jax
import jax.numpy as jnp
from jax.experimental.layout import Layout, with_layout_constraint
from jax import lax
from jax.experimental import pallas as pl
from jax.experimental.pallas import tpu as pltpu
from jax.sharding import PartitionSpec as P

F32 = jnp.float32
BF16 = jnp.bfloat16
ANY = pl.BlockSpec(memory_space=pl.ANY)


def attention_kernel(first, q_ref, kv_ref, *rest):
    o_ref, q_rows, m_ref, l_ref, acc_ref = rest[-5:]
    i = pl.program_id(0) + first
    ring = kv_ref.shape[0]
    blk = kv_ref.shape[3]
    per_q, hd = q_ref.shape[0], q_ref.shape[1]
    scale = math.log2(math.e) / math.sqrt(hd)
    for u in range(per_q):
        q_rows[u * blk:(u + 1) * blk, :] = q_ref[u].T
    m_ref[...] = jnp.full(m_ref.shape, -jnp.inf, F32)
    l_ref[...] = jnp.zeros(l_ref.shape, F32)
    acc_ref[...] = jnp.zeros(acc_ref.shape, F32)

    half = q_rows.shape[0] // 2

    def step(start, count, spans, masked):
        keys, values = [], []
        for u in range(count):
            b = start + u
            keys.append(kv_ref[lax.rem(b, ring), lax.div(b, ring), :hd, :])
            values.append(kv_ref[lax.rem(b, ring), lax.div(b, ring), hd:, :])
        k = jnp.concatenate(keys, axis=1)
        v = jnp.concatenate(values, axis=1)
        scores = [jnp.dot(q_rows[span, :], k, preferred_element_type=F32) for span in spans]
        for span, s in zip(spans, scores):
            if masked:
                row = lax.broadcasted_iota(jnp.int32, s.shape, 0) + span.start
                col = lax.broadcasted_iota(jnp.int32, s.shape, 1)
                s = jnp.where(row >= col, s, -jnp.inf)
            pieces = [s[:, u:u + hd] for u in range(0, count * blk, hd)]
            m_old = m_ref[span, :]
            top = functools.reduce(jnp.maximum, pieces)
            m_new = jnp.maximum(m_old, jnp.max(top, axis=1, keepdims=True))
            m_ref[span, :] = m_new
            alpha = jnp.exp2((m_old - m_new) * scale)
            m_scaled = m_new * scale
            parts = [jnp.exp2(piece * scale - m_scaled) for piece in pieces]
            l_ref[span, :] = l_ref[span, :] * alpha + functools.reduce(jnp.add, parts)
            p = jnp.concatenate([part.astype(BF16) for part in parts], axis=1)
            o = lax.dot_general(p, v, (((1,), (1,)), ((), ())), preferred_element_type=F32)
            acc_ref[span, :] = acc_ref[span, :] * alpha + o

    def full(j, carry):
        step(j * per_q, per_q, [slice(0, half), slice(half, 2 * half)], False)
        return carry

    lax.fori_loop(0, i, full, 0)
    step(i * per_q, per_q, [slice(0, half), slice(half, 2 * half)], True)
    o_ref[...] = (acc_ref[...] / jnp.sum(l_ref[...], axis=1, keepdims=True)).astype(BF16)


def attention(q, kv, lo, hi, per_q, into=None, after=()):
    n_src, hd, blk = q.shape
    ring, rows = kv.shape[:2]
    q_block = per_q * blk
    seq = n_src * blk
    extra = list(after) + ([into] if into is not None else [])
    pairs = (hi * hi - lo * lo) * q_block * q_block / 2
    return pl.pallas_call(
        functools.partial(attention_kernel, lo),
        grid=(hi - lo,),
        in_specs=[
            pl.BlockSpec((per_q, hd, blk), lambda i: (i + lo, 0, 0)),
            pl.BlockSpec((ring, rows, 2 * hd, blk), lambda i: (0, 0, 0, 0)),
        ] + [ANY] * len(extra),
        out_specs=pl.BlockSpec((q_block, hd), lambda i: (i + lo, 0)),
        out_shape=jax.ShapeDtypeStruct((seq, hd), BF16),
        scratch_shapes=[pltpu.VMEM((q_block, hd), BF16)] + [pltpu.VMEM((q_block, hd), F32)] * 3,
        input_output_aliases={1 + len(extra): 0} if into is not None else {},
        cost_estimate=pl.CostEstimate(flops=int(4 * hd * pairs * 2), bytes_accessed=int(seq * hd * 8), transcendentals=int(pairs)),
        name='attend',
    )(q, kv, *extra)


def project_kernel(heads_blk, parts, o_ref, w_ref, x_ref, ids_ref, wr_ref, *rest):
    *part_refs, h_ref, g_ref, acc_ref = rest[-3 - parts:]
    step = pl.program_id(0)

    @pl.when(step == 0)
    def _():
        acc_ref[...] = jnp.zeros(acc_ref.shape, F32)

    o = jnp.concatenate([o_ref[u] for u in range(heads_blk)], axis=1)
    tile = min(w_ref.shape[2], 512)

    def add(c, carry):
        cols = pl.ds(pl.multiple_of(c * tile, tile), tile)
        w = w_ref[:, :, cols].reshape(heads_blk * w_ref.shape[1], tile)
        acc_ref[:, cols] += jnp.dot(o, w, preferred_element_type=F32)
        return carry

    lax.fori_loop(0, w_ref.shape[2] // tile, add, 0)

    @pl.when(step == pl.num_programs(0) - 1)
    def _():
        h = (x_ref[...].astype(F32) + acc_ref[...]).astype(BF16)
        h_ref[...] = h
        for u, part_ref in enumerate(part_refs):
            size = part_ref.shape[1]
            part_ref[...] = h[:, u * size:(u + 1) * size]
        logits = jnp.dot(h, wr_ref[...], preferred_element_type=F32)
        expert = lax.broadcasted_iota(jnp.int32, logits.shape, 1)
        chosen = ids_ref[:, 0:1] == expert
        for u in range(1, ids_ref.shape[1]):
            chosen = jnp.logical_or(chosen, ids_ref[:, u:u + 1] == expert)
        picked = jnp.where(chosen, logits, -jnp.inf)
        e = jnp.exp(picked - jnp.max(picked, axis=1, keepdims=True))
        g_ref[...] = (e / jnp.sum(e, axis=1, keepdims=True)).T


def project(o, w_out, x, ids, w_router, parts, after=()):
    heads, tok, hd = o.shape
    width = w_out.shape[2]
    experts = w_router.shape[1]
    heads_blk = min(heads, 8)
    return pl.pallas_call(
        functools.partial(project_kernel, heads_blk, parts),
        grid=(heads // heads_blk,),
        in_specs=[
            pl.BlockSpec((heads_blk, tok, hd), lambda i: (i, 0, 0)),
            pl.BlockSpec((heads_blk, hd, width), lambda i: (i, 0, 0)),
            pl.BlockSpec((tok, width), lambda i: (0, 0)),
            pl.BlockSpec((tok, ids.shape[1]), lambda i: (0, 0)),
            pl.BlockSpec((width, experts), lambda i: (0, 0)),
        ] + [ANY] * len(after),
        out_specs=[pl.BlockSpec((tok, width // parts), lambda i: (0, 0))] * parts + [
            pl.BlockSpec((tok, width), lambda i: (0, 0)),
            pl.BlockSpec((experts, tok), lambda i: (0, 0)),
        ],
        out_shape=[jax.ShapeDtypeStruct((tok, width // parts), BF16)] * parts + [
            jax.ShapeDtypeStruct((tok, width), BF16), jax.ShapeDtypeStruct((experts, tok), F32)],
        scratch_shapes=[pltpu.VMEM((tok, width), F32)],
        cost_estimate=pl.CostEstimate(flops=2 * tok * heads * hd * width, bytes_accessed=heads * hd * width * 2, transcendentals=0),
        name='project',
    )(o, w_out, x, ids, w_router, *after)


def rows_kernel(h_ref, rank_ref, gate_ref, *rest):
    out_ref = rest[-1]
    experts = out_ref.shape[1]
    some, _, tok = gate_ref.shape
    cap = out_ref.shape[2] // some
    slot = lax.broadcasted_iota(jnp.int32, (cap, tok), 0).astype(F32)

    def source(u, carry):
        hot, gate = [], []
        for e in range(experts):
            here = rank_ref[u, 0, e:e + 1, :] == slot
            hot.append(jnp.where(here, 1.0, 0.0))
            gate.append(jnp.sum(jnp.where(here, gate_ref[u, e:e + 1, :], 0.0), axis=1, keepdims=True))
        select = jnp.concatenate(hot, axis=0).astype(BF16)
        gates = jnp.concatenate(gate, axis=0)
        rows = jnp.dot(select, h_ref[pl.ds(pl.multiple_of(u * tok, tok), tok), :], preferred_element_type=F32)
        slots = pl.ds(pl.multiple_of(u * cap, cap), cap)
        out_ref[0, :, slots, :] = (rows * gates).astype(BF16).reshape(experts, cap, rows.shape[1])
        return carry

    lax.fori_loop(0, some, source, 0)


def expert_rows(h_all, ranks, gates, micro, cap, width, column, into=None, after=()):
    sources, n_micro, experts, tok = ranks.shape
    part = h_all.shape[1]
    some = min(sources, 4)
    extra = list(after) + ([into] if into is not None else [])
    return pl.pallas_call(
        rows_kernel,
        grid=(sources // some,),
        in_specs=[
            pl.BlockSpec((some * tok, part), lambda s: (s, 0)),
            pl.BlockSpec((some, 1, experts, tok), lambda s: (s, micro, 0, 0)),
            pl.BlockSpec((some, experts, tok), lambda s: (s, 0, 0)),
        ] + [ANY] * len(extra),
        out_specs=pl.BlockSpec((1, experts, some * cap, part), lambda s: (micro, 0, s, column)),
        out_shape=jax.ShapeDtypeStruct((n_micro, experts, sources * cap, width), BF16),
        input_output_aliases={2 + len(extra): 0} if into is not None else {},
        cost_estimate=pl.CostEstimate(flops=2 * sources * experts * cap * tok * part, bytes_accessed=2 * sources * (tok + experts * cap) * part, transcendentals=0),
        name='expert_rows',
    )(h_all, ranks, gates, *extra)


def slot_ranks(ids, experts, cap):
    tok = ids.shape[1]
    hot = jnp.any(ids[:, None, :, :] == jnp.arange(experts)[None, :, None, None], axis=-1)
    earlier = (jnp.arange(tok)[:, None] < jnp.arange(tok)[None, :]).astype(BF16)
    rank = jnp.einsum('met,ts->mes', hot.astype(BF16), earlier, preferred_element_type=F32)
    return jnp.where(jnp.logical_and(hot, rank < cap), rank, -1.0)


def solution(mesh):
    groups = mesh.shape['sp']

    def local_step(tokens, expert_ids, w_query, w_key, w_value, w_out, w_router):
        n_micro, tok, width = tokens.shape
        top_k = expert_ids.shape[2]
        heads, hd = w_query.shape[1:]
        kv_heads = w_key.shape[1]
        experts = w_router.shape[1]
        own = experts // groups
        cap = 2 * tok * top_k // experts
        share = groups // kv_heads
        seq = groups * tok
        columns = [[r + share * y for y in range(kv_heads)] for r in range(share)]
        rows = [[r + share * y for r in range(share)] for y in range(kv_heads)]
        per_q = min(4, groups)
        n_blk = groups // per_q

        def swap(a, **kw):
            return lax.all_to_all(a, 'sp', 0, 0, tiled=True, **kw)

        w_kv = jnp.concatenate([w_key, w_value], axis=2)
        kv = jnp.einsum('mtd,dhk->hmkt', tokens, w_kv, preferred_element_type=F32).astype(BF16)
        ranks = slot_ranks(expert_ids, experts, cap).reshape(n_micro, groups, own, tok).transpose(1, 0, 2, 3)
        mine = swap(kv, axis_index_groups=columns)
        queries = jnp.einsum('mtd,dhk->hmkt', tokens, w_query, preferred_element_type=F32).astype(BF16)
        queries = with_layout_constraint(queries, Layout(major_to_minor=(0, 1, 2, 3)))
        mine, queries, ranks = lax.optimization_barrier((mine, queries, ranks))
        ranks = swap(ranks)
        kv_held, q_held = [], []
        for m in range(n_micro):
            q = queries[:, m]
            if m > 0:
                q, _ = lax.optimization_barrier((q, q_held[-1]))
            gathered = lax.all_gather(mine[:, m], 'sp', axis=0, axis_index_groups=rows)
            kv_held.append(gathered.reshape(share, kv_heads, 2 * hd, tok))
            q_held.append(swap(q))

        hidden, buffers, gathered = [], None, []
        attn = attention(q_held[0], kv_held[0], 0, n_blk, per_q)
        for m in range(n_micro):
            o = swap(attn.reshape(groups, tok, hd))
            part = None
            last = m + 1 == n_micro
            if not last:
                cut = (5 * n_blk) // 8
                part = attention(q_held[m + 1], kv_held[m + 1], 0, cut, per_q)
            parts = 1
            *pieces, h, gate = project(o, w_out, tokens[m], expert_ids[m], w_router, parts, after=() if last else (part,))
            hidden.append(h)
            pieces = [lax.all_gather(piece, 'sp', axis=0, tiled=True) for piece in pieces]
            gates = swap(gate.reshape(groups, own, tok))
            gathered.append((pieces, gates))
            if not last:
                attn = attention(q_held[m + 1], kv_held[m + 1], cut, n_blk, per_q, into=part, after=(h,))
        for m in range(n_micro):
            pieces, gates = gathered[m]
            for c, piece in enumerate(pieces):
                buffers = expert_rows(piece, ranks, gates, m, cap, width, c, into=buffers, after=(attn,) if m == 0 else ())
        return jnp.stack(hidden), buffers

    return jax.shard_map(
        local_step,
        mesh=mesh,
        in_specs=(P('dp', 'sp', None), P('dp', 'sp', None), P(), P(), P(), P(), P()),
        out_specs=(P('dp', 'sp', None), P('dp', 'sp', None, None)),
        check_vma=False,
    )
```
